32 devices in a mesh: leaf: 32 (over z, y, x, core).
Axes of the slice: x: 2, y: 2, z: 4, core: 2. Of those that a mesh axis runs over, the one named last changes fastest.
Arguments:
- slip: bfloat16 [128, 8192], P(None, 'leaf'), may hold values from -6 to 6
- to_multipole: bfloat16 [121, 128], replicated, may hold values from -0.5 to 0.5
- up_shift: float32 [2, 121, 121], replicated, may hold values from -0.375 to 0.375
- down_shift: float32 [2, 121, 121], replicated, may hold values from -0.5 to 0.5
- sibling_far: float32 [2, 121, 121], replicated, may hold values from -0.5 to 0.5
- leaf_far: bfloat16 [27, 121, 121], replicated, may hold values from -0.25 to 0.25
- to_stress: bfloat16 [128, 121], replicated, may hold values from -0.125 to 0.125
- near_blocks: bfloat16 [9, 128, 128], replicated, may hold values from -0.1875 to 0.1875
- send_cells: int32 [32, 4096], P('leaf'), may hold values from 0 to 255, as said below
- far_list: int32 [27, 8192], P(None, 'leaf'), may hold values from 0 to 4351, as said below
- near_list: int32 [9, 8192], P(None, 'leaf'), may hold values from 0 to 319, as said below
Outputs:
- stress: float32 [128, 8192], P(None, 'leaf')
The draws below stay inside these ranges and needn't reach their ends.
Inputs may be any that keep to these rules, and one draw needn't show every extreme that they name: `send_cells`: row q holds, in positions d * 128 to (d + 1) * 128 - 1, 128 distinct cells of device q (numbered within that device) listed for receiving device d. `far_list`: an entry v below 256 names a cell of the target's own device. Otherwise v - 256 = q * 128 + s names slot s of device q's list for the target's device, q is not the target's device, s < 128 when q lies within 4 devices of it and s < 32 when it lies farther; in every draw some entry names slot 127 of a device within 4, and some names slot 31 of a farther device. `near_list`: an entry w names the cell w - 32 counted from the first cell of the target's device, so that positions before 0 and from 256 on lie on the neighbouring devices (zeros outside the fault); entry 4 is the target itself.
All inputs are finite; a program needn't handle non-finite values.
Results may differ from the reference program's by a relative error of at most 0.0031.
Values may be sent and summed in bfloat16 or wider, within the bound.
A program may use at most 64 MiB of HBM per device.

```python
import jax
import jax.numpy as jnp
from jax import lax

ELEM = 128
COEF = 121
NEAR = 9
TYPES = 27
NEAR_PEERS = 4
CELLS_DEV = 256
HALO = 32
CAP_NEAR = 128
CAP_FAR = 32
CELLS = 8192
N_LEAF = 32


def let_plan(key):
    base = jax.random.fold_in(key, 4127)
    keys = jax.random.split(base, 5)
    devices_all = N_LEAF
    receiver = jnp.arange(devices_all, dtype=jnp.int32)[:, None]
    sender = jnp.arange(devices_all, dtype=jnp.int32)[None, :]
    apart = jnp.abs(sender - receiver)
    close_count = jax.random.randint(keys[0], (devices_all, devices_all), CAP_NEAR // 4, CAP_NEAR + 1)
    far_count = jax.random.randint(keys[1], (devices_all, devices_all), CAP_FAR // 2, CAP_FAR + 1)
    counts = jnp.where(apart == 0, 0, jnp.where(apart <= NEAR_PEERS, close_count, far_count))
    counts = jnp.where(sender == receiver + 1, CAP_NEAR, counts)
    counts = jnp.where(sender == (receiver + devices_all // 2) % devices_all, CAP_FAR, counts)
    scores = jax.random.randint(keys[2], (devices_all, devices_all, CELLS_DEV), 0, 1 << 20)
    scores = scores * CELLS_DEV + jnp.arange(CELLS_DEV, dtype=jnp.int32)
    chosen = jnp.argsort(scores, axis=-1)[:, :, :CAP_NEAR].astype(jnp.int32)
    send_lists = chosen.reshape(devices_all, devices_all * CAP_NEAR)
    entries = TYPES * CELLS_DEV
    position = jnp.arange(CAP_NEAR, dtype=jnp.int32)
    usable = (position[None, None, :] < counts[:, :, None]).reshape(devices_all, devices_all * CAP_NEAR)
    codes = CELLS_DEV + jnp.arange(devices_all * CAP_NEAR, dtype=jnp.int32)
    ranks = jnp.cumsum(usable.astype(jnp.int32), axis=1) - 1
    place_scores = jax.random.randint(keys[3], (devices_all, entries - 1), 0, 1 << 14)
    place_scores = place_scores * entries + jnp.arange(entries - 1, dtype=jnp.int32)
    places = 1 + jnp.argsort(place_scores, axis=1).astype(jnp.int32)
    targets = jnp.take_along_axis(places, jnp.clip(ranks, 0, entries - 2), axis=1)
    targets = jnp.where(usable, targets, entries)
    own_cells = jax.random.randint(keys[4], (devices_all, entries), 0, CELLS_DEV)
    own_cells = own_cells.at[:, 0].set(0)
    rows = jnp.broadcast_to(receiver, targets.shape)
    filled = own_cells.at[rows, targets].set(jnp.broadcast_to(codes[None, :], targets.shape), mode='drop')
    lists = filled.reshape(devices_all, TYPES, CELLS_DEV).transpose(1, 0, 2).reshape(TYPES, devices_all * CELLS_DEV)
    return (send_lists.astype(jnp.int32), lists.astype(jnp.int32))


def draw_send_cells(key, part):
    return let_plan(key)[0]


def draw_far_list(key, part):
    return let_plan(key)[1]


def draw_near_list(key, part):
    base = jax.random.fold_in(key, 9151)
    cells_here = jnp.arange(CELLS_DEV, dtype=jnp.int32)
    jumps = jax.random.randint(base, (NEAR, N_LEAF, CELLS_DEV), -HALO, HALO + 1)
    kinds = jnp.arange(NEAR, dtype=jnp.int32)[:, None, None]
    jumps = jnp.where(kinds == NEAR // 2, 0, jumps)
    values = cells_here[None, None, :] + HALO + jumps
    values = values.at[0, :, 0].set(0)
    values = values.at[NEAR - 1, :, CELLS_DEV - 1].set(CELLS_DEV + 2 * HALO - 1)
    return values.reshape(NEAR, N_LEAF * CELLS_DEV).astype(jnp.int32)


def level_of(stream_key, extent, cuts, least, largest):
    def one(dim, shards_of):
        steps = jax.random.uniform(jax.random.fold_in(jax.random.fold_in(stream_key, 6), dim), (shards_of,), jnp.float32, least / len(cuts), largest / len(cuts))
        return jnp.repeat(jnp.exp(steps), extent[dim] // shards_of).reshape((-1,) + (1,) * (len(extent) - dim - 1))

    loudness = one(*cuts[0])
    for cut in cuts[1:]:
        loudness = loudness * one(*cut)
    return loudness


def noise(stream_key, dims, spread, bound, pieces=(), kind=jnp.bfloat16):
    values = spread * jax.random.normal(stream_key, dims, jnp.float32)
    if pieces:
        values = values * level_of(stream_key, dims, pieces, -0.22, 0.18)
    return jnp.clip(values, -bound, bound).astype(kind)


def setup_inputs(seed: int = 0) -> dict:
    key_of = jax.random.split(jax.random.key(seed), 12)
    return {
        "slip": noise(key_of[0], (ELEM, CELLS), 1.0, 6.0, ((1, 32),)),
        "to_multipole": noise(key_of[1], (COEF, ELEM), ELEM ** -0.5, 0.5),
        "up_shift": noise(key_of[2], (2, COEF, COEF), (2 * COEF) ** -0.5, 0.375, (), jnp.float32),
        "down_shift": noise(key_of[3], (2, COEF, COEF), COEF ** -0.5, 0.5, (), jnp.float32),
        "sibling_far": noise(key_of[4], (2, COEF, COEF), COEF ** -0.5, 0.5, (), jnp.float32),
        "leaf_far": noise(key_of[5], (TYPES, COEF, COEF), (4 * COEF) ** -0.5, 0.25),
        "to_stress": noise(key_of[6], (ELEM, COEF), (16 * COEF) ** -0.5, 0.125),
        "near_blocks": noise(key_of[7], (NEAR, ELEM, ELEM), (NEAR * ELEM) ** -0.5, 0.1875),
        "send_cells": draw_send_cells(jax.random.fold_in(key_of[11], 71), 0),
        "far_list": draw_far_list(jax.random.fold_in(key_of[11], 71), 0),
        "near_list": draw_near_list(jax.random.fold_in(key_of[11], 71), 0),
    }


def reference(slip, to_multipole, up_shift, down_shift, sibling_far, leaf_far, to_stress, near_blocks, send_cells, far_list, near_list):
    precise = lax.Precision.HIGHEST
    multipole = jnp.dot(to_multipole, slip, preferred_element_type=jnp.float32).astype(jnp.bfloat16)
    heights = CELLS.bit_length() - 1
    aggregates = [multipole.astype(jnp.float32)]
    for height in range(heights - 1):
        below = aggregates[-1]
        aggregates.append(jnp.dot(up_shift[0], below[:, 0::2], precision=precise)
                          + jnp.dot(up_shift[1], below[:, 1::2], precision=precise))
    expansion = jnp.zeros((COEF, 1), jnp.float32)
    for height in range(heights - 1, -1, -1):
        left_part = jnp.dot(down_shift[0], expansion, precision=precise)
        right_part = jnp.dot(down_shift[1], expansion, precision=precise)
        if height >= 1:
            level_sums = aggregates[height]
            left_part = left_part + jnp.dot(sibling_far[0], level_sums[:, 1::2], precision=precise)
            right_part = right_part + jnp.dot(sibling_far[1], level_sums[:, 0::2], precision=precise)
        expansion = jnp.stack([left_part, right_part], axis=-1).reshape(COEF, -1)
    owner = jnp.arange(CELLS, dtype=jnp.int32) // CELLS_DEV
    relative = far_list - CELLS_DEV
    sender = jnp.clip(relative // CAP_NEAR, 0, N_LEAF - 1).astype(jnp.int32)
    position = (relative % CAP_NEAR).astype(jnp.int32)
    flat_lists = send_cells.reshape(-1)
    listed = flat_lists[sender * (N_LEAF * CAP_NEAR) + owner[None, :] * CAP_NEAR + position]
    source = jnp.where(far_list < CELLS_DEV, owner[None, :] * CELLS_DEV + far_list, sender * CELLS_DEV + listed).astype(jnp.int32)
    leaf_sum = jnp.zeros((COEF, CELLS), jnp.float32)
    for kind in range(TYPES):
        leaf_sum = leaf_sum + jnp.dot(leaf_far[kind], jnp.take(multipole, source[kind], axis=1), preferred_element_type=jnp.float32)
    local_exp = (expansion + leaf_sum).astype(jnp.bfloat16)
    padded = jnp.pad(slip, ((0, 0), (HALO, HALO)))
    near_source = (owner[None, :] * CELLS_DEV + near_list).astype(jnp.int32)
    stress = jnp.dot(to_stress, local_exp, preferred_element_type=jnp.float32)
    for kind in range(NEAR):
        stress = stress + jnp.dot(near_blocks[kind], jnp.take(padded, near_source[kind], axis=1), preferred_element_type=jnp.float32)
    return stress
```

```python
import functools

import jax
import jax.numpy as jnp
from jax import lax
from jax.experimental import pallas as pl
from jax.experimental.pallas import tpu as pltpu
from jax.sharding import PartitionSpec as P

HALO = 32
PEERS = 4
CAP_FAR = 32
LANES = 128
BF = jnp.bfloat16
F32 = jnp.float32
MESH = pl.DeviceIdType.MESH
OFFSETS = tuple(range(-PEERS, 0)) + tuple(range(1, PEERS + 1))


def mm(a, b):
    return jnp.dot(a, b, preferred_element_type=F32)


def halves(x):
    high = x.astype(BF)
    return high, (x - high.astype(F32)).astype(BF)


def one_hot(rows, index):
    count = index.shape[1]
    lines = lax.broadcasted_iota(jnp.int32, (rows, count), 0).astype(F32).astype(BF)
    hit = lines == jnp.broadcast_to(index.astype(BF), (rows, count))
    return jnp.where(hit, jnp.ones((), BF), jnp.zeros((), BF))


def kernel(
    n, cells, cap,
    slip_ref, tm_ref, up_ref, down_ref, sib_ref, leaf_ref, ts_ref, nb_ref, send_ref, far_ref, near_ref,
    out_ref,
    outgoing, far_buf, near_buf, edges, halo, root_out, roots,
    weight, w_up, w_sib, w_down, agg, terms, loc, rel, near_rel, source,
    far_send, far_recv, near_send, near_recv, halo_send, halo_recv, root_send, root_recv,
):
    me = lax.axis_index("leaf")
    coef = tm_ref.shape[0]
    types = far_ref.shape[0]
    kinds = near_ref.shape[0]
    rest = cap - CAP_FAR

    barrier = pltpu.get_barrier_semaphore()

    far_buf[...] = jnp.zeros_like(far_buf)
    near_buf[...] = jnp.zeros_like(near_buf)
    halo[...] = jnp.zeros_like(halo)

    def greet(k, carry):
        pl.semaphore_signal(barrier, inc=1, device_id=(lax.rem(me + k, n),), device_id_type=MESH)
        return carry

    lax.fori_loop(1, n, greet, 0)

    edges[0] = slip_ref[:, :LANES].astype(F32).T[:HALO].astype(BF)
    edges[1] = slip_ref[:, cells - LANES :].astype(F32).T[LANES - HALO :].astype(BF)

    weight[...] = jnp.zeros_like(weight)
    weight[0, :coef, :] = tm_ref[...].astype(F32)
    multipole = mm(weight[0].astype(BF), slip_ref[...]).astype(BF)
    source[:, :cells] = multipole

    chunk = 4 * cap
    for start in range(0, n * cap, chunk):
        picked = one_hot(cells, send_ref[0:1, start : start + chunk].astype(F32))
        outgoing[start : start + chunk, :] = mm(multipole, picked).T.astype(BF)

    pl.semaphore_wait(barrier, n - 1)

    def far_copy(k):
        target = lax.rem(me + k, n)
        return pltpu.make_async_remote_copy(
            src_ref=outgoing.at[pl.ds(pl.multiple_of(target * cap, cap), CAP_FAR)],
            dst_ref=far_buf.at[pl.ds(pl.multiple_of(me * CAP_FAR, CAP_FAR), CAP_FAR)],
            send_sem=far_send.at[k],
            recv_sem=far_recv.at[k],
            device_id=(target,),
            device_id_type=MESH,
        )

    def near_copy(j):
        target = jnp.clip(me + OFFSETS[j], 0, n - 1)
        back = len(OFFSETS) - 1 - j
        return pltpu.make_async_remote_copy(
            src_ref=outgoing.at[pl.ds(pl.multiple_of(target * cap + CAP_FAR, CAP_FAR), rest)],
            dst_ref=near_buf.at[pl.ds(back * rest, rest)],
            send_sem=near_send.at[j],
            recv_sem=near_recv.at[back],
            device_id=(target,),
            device_id_type=MESH,
        )

    def halo_copy(side):
        target = jnp.clip(me + (1 if side else -1), 0, n - 1)
        return pltpu.make_async_remote_copy(
            src_ref=edges.at[side],
            dst_ref=halo.at[pl.ds((1 - side) * HALO, HALO)],
            send_sem=halo_send.at[side],
            recv_sem=halo_recv.at[1 - side],
            device_id=(target,),
            device_id_type=MESH,
        )

    def root_copy(k):
        return pltpu.make_async_remote_copy(
            src_ref=root_out,
            dst_ref=roots.at[pl.ds(pl.multiple_of(me * 8, 8), 8)],
            send_sem=root_send.at[k],
            recv_sem=root_recv.at[k],
            device_id=(lax.rem(me + k, n),),
            device_id_type=MESH,
        )

    def inside(offset):
        return jnp.logical_and(me + offset >= 0, me + offset < n)

    for side in (0, 1):
        @pl.when(inside(1 if side else -1))
        def _():
            halo_copy(side).start()

    def start_far(k, carry):
        far_copy(k).start()
        return carry

    lax.fori_loop(1, n, start_far, 0)
    for j, offset in enumerate(OFFSETS):
        @pl.when(inside(offset))
        def _():
            near_copy(j).start()

    def parts(ref, index):
        weight[index, :coef, :coef] = ref
        weight[index, :coef, coef:] = jnp.zeros((coef, LANES - coef), F32)
        return halves(weight[index].T)

    w_sib[...] = jnp.zeros_like(w_sib)
    for s in (0, 1):
        high, low = parts(up_ref[s], 0 + s)
        w_up[s * LANES : (s + 1) * LANES, :LANES] = high
        w_up[s * LANES : (s + 1) * LANES, LANES:] = low
        high, low = parts(down_ref[s], 2 + s)
        w_down[:LANES, s * LANES : (s + 1) * LANES] = high
        w_down[LANES:, s * LANES : (s + 1) * LANES] = low
        high, low = parts(sib_ref[s], 4 + s)
        other = 1 - s
        w_sib[0, other * LANES : (other + 1) * LANES, s * LANES : (s + 1) * LANES] = high
        w_sib[1, other * LANES : (other + 1) * LANES, s * LANES : (s + 1) * LANES] = low

    def pair(base, rows):
        m = max(rows // 2, 8)
        even = agg[pl.ds(base, m, stride=2), :]
        odd = agg[pl.ds(base + 1, m, stride=2), :]
        return m, halves(jnp.concatenate([even, odd], axis=1))

    def lift(high, low):
        first = mm(high, w_up[...])
        second = mm(low, w_up[:, :LANES])
        return first[:, :LANES] + first[:, LANES:] + second

    def across(high, low):
        return mm(high, w_sib[0]) + mm(high, w_sib[1]) + mm(low, w_sib[0])

    def place(base, value):
        agg[base : base + value.shape[0], :] = value
        if value.shape[0] < 16:
            agg[base + value.shape[0] : base + 16, :] = jnp.zeros((16 - value.shape[0], LANES), F32)

    local_levels = cells.bit_length() - 1
    tree_bits = n.bit_length() - 1
    base, spot = 0, 0
    agg[:cells, :] = multipole.astype(F32).T
    local_spots = []
    for height in range(local_levels):
        rows = cells >> height
        m, (high, low) = pair(base, rows)
        if height >= 1:
            terms[spot : spot + m, :] = across(high, low)
            local_spots.append(spot)
            spot += m
        else:
            local_spots.append(None)
        value = lift(high, low)
        base += max(rows, 16)
        place(base, value)
    root_out[...] = value
    roots[pl.ds(pl.multiple_of(me * 8, 8), 8), :] = value

    def start_root(k, carry):
        root_copy(k).start()
        return carry

    lax.fori_loop(1, n, start_root, 0)

    v = far_ref[...]
    behind = v - cells
    sender = behind // cap
    slot = behind % cap
    delta = sender - me
    lane = jnp.where(delta < 0, delta + PEERS, delta + PEERS - 1)
    position = jnp.where(
        v < cells,
        v,
        jnp.where(
            slot < CAP_FAR,
            cells + sender * CAP_FAR + slot,
            cells + n * CAP_FAR + lane * rest + slot - CAP_FAR,
        ),
    )
    total = source.shape[1]
    blocks = total // 256
    for b in range(blocks):
        rel[b, :types, :] = jnp.clip(position - 256 * b, -1, 256).astype(F32)

    for side in (0, 1):
        @pl.when(inside(1 if side else -1))
        def _():
            halo_copy(side).wait_send()

        @pl.when(inside(-1 if side else 1))
        def _():
            halo_copy(side).wait_recv()

    w = near_ref[...]
    near_rel[0, :kinds, :] = jnp.clip(w - HALO, -1, cells).astype(F32)
    near_rel[1, :kinds, :] = jnp.where(
        w < HALO, w, jnp.where(w >= HALO + cells, w - cells, -1)
    ).astype(F32)
    slips = slip_ref[...]
    side_slips = jnp.concatenate(
        [halo[...], jnp.zeros((LANES - 2 * HALO, LANES), BF)], axis=0
    ).astype(F32).T.astype(BF)
    stress = jnp.zeros(out_ref.shape, F32)
    for k in range(kinds):
        column = mm(slips, one_hot(cells, near_rel[0, k : k + 1, :])) + mm(
            side_slips, one_hot(LANES, near_rel[1, k : k + 1, :])
        )
        stress = stress + mm(nb_ref[k], column.astype(BF))
    out_ref[...] = stress

    def wait_root(k, carry):
        root_copy(k).wait()
        return carry

    lax.fori_loop(1, n, wait_root, 0)
    base = 0
    place(base, roots[pl.ds(0, n, stride=8), :])
    tree_spots = []
    for bit in range(tree_bits):
        rows = n >> bit
        m, (high, low) = pair(base, rows)
        terms[spot : spot + m, :] = across(high, low)
        tree_spots.append(spot)
        spot += m
        if bit + 1 < tree_bits:
            value = lift(high, low)
            base += max(rows, 16)
            place(base, value)

    def descend(x):
        high, low = halves(x)
        return mm(high, w_down[:LANES, :]) + mm(high, w_down[LANES:, :]) + mm(low, w_down[:LANES, :])

    expansion = jnp.zeros((8, LANES), F32)
    for bit in reversed(range(tree_bits)):
        both = terms[pl.ds(tree_spots[bit] + (me >> (bit + 1)), 1), :]
        both = jnp.broadcast_to(both, (8, 2 * LANES))
        if bit + 1 < tree_bits:
            both = both + descend(expansion)
        expansion = jnp.where((me >> bit) & 1 == 0, both[:, :LANES], both[:, LANES:])
    for height in reversed(range(local_levels)):
        m = max((cells >> height) // 2, 8)
        both = descend(expansion)
        if height >= 1:
            both = both + terms[local_spots[height] : local_spots[height] + m, :]
        loc[pl.ds(0, m, stride=2), :] = both[:, :LANES]
        loc[pl.ds(1, m, stride=2), :] = both[:, LANES:]
        expansion = loc[: max(cells >> height, 8), :]

    def wait_far(k, carry):
        far_copy(k).wait()
        return carry

    lax.fori_loop(1, n, wait_far, 0)
    for j, offset in enumerate(OFFSETS):
        @pl.when(inside(offset))
        def _():
            near_copy(j).wait_send()

        @pl.when(inside(OFFSETS[len(OFFSETS) - 1 - j]))
        def _():
            near_copy(j).wait_recv()

    far_end = cells + n * CAP_FAR
    source[:, cells:far_end] = far_buf[...].astype(F32).T.astype(BF)
    source[:, far_end:] = near_buf[...].astype(F32).T.astype(BF)

    def leaf(t, acc):
        hits = jnp.concatenate(
            [one_hot(256, rel[b, pl.ds(t, 1), :]) for b in range(blocks)], axis=0
        )
        column = mm(source[...], hits).astype(BF)
        return acc + mm(leaf_ref[t], column[:coef])

    leaf_sum = lax.fori_loop(0, types, leaf, jnp.zeros((coef, cells), F32))
    local_exp = (expansion.T[:coef] + leaf_sum).astype(BF)
    out_ref[...] = out_ref[...] + mm(ts_ref[...], local_exp)


def round_up(value, unit):
    return -(-value // unit) * unit


def body(*args):
    slip, to_multipole, _, _, _, _, _, _, send_cells, far_list, near_list = args
    n = lax.axis_size("leaf")
    cells = slip.shape[1]
    cap = send_cells.shape[1] // n
    rest = cap - CAP_FAR
    peers = len(OFFSETS)
    total = cells + n * CAP_FAR + peers * rest
    dma = pltpu.SemaphoreType.DMA
    return pl.pallas_call(
        functools.partial(kernel, n, cells, cap),
        out_shape=jax.ShapeDtypeStruct(slip.shape, F32),
        in_specs=[pl.BlockSpec(memory_space=pltpu.VMEM)] * len(args),
        out_specs=pl.BlockSpec(memory_space=pltpu.VMEM),
        scratch_shapes=[
            pltpu.VMEM((n * cap, LANES), BF),
            pltpu.VMEM((n * CAP_FAR, LANES), BF),
            pltpu.VMEM((peers * rest, LANES), BF),
            pltpu.VMEM((2, HALO, LANES), BF),
            pltpu.VMEM((2 * HALO, LANES), BF),
            pltpu.VMEM((8, LANES), F32),
            pltpu.VMEM((n * 8, LANES), F32),
            pltpu.VMEM((6, LANES, LANES), F32),
            pltpu.VMEM((2 * LANES, 2 * LANES), BF),
            pltpu.VMEM((2, 2 * LANES, 2 * LANES), BF),
            pltpu.VMEM((2 * LANES, 2 * LANES), BF),
            pltpu.VMEM((2 * cells + 2 * n + 128, LANES), F32),
            pltpu.VMEM((cells + n + 128, 2 * LANES), F32),
            pltpu.VMEM((cells, LANES), F32),
            pltpu.VMEM((total // 256, round_up(far_list.shape[0], 8), cells), F32),
            pltpu.VMEM((2, round_up(near_list.shape[0], 8), cells), F32),
            pltpu.VMEM((LANES, total), BF),
            dma((n,)),
            dma((n,)),
            dma((peers,)),
            dma((peers,)),
            dma((2,)),
            dma((2,)),
            dma((n,)),
            dma((n,)),
        ],
        compiler_params=pltpu.CompilerParams(collective_id=0, has_side_effects=True),
    )(*args)


def solution(mesh):
    return jax.shard_map(
        body,
        mesh=mesh,
        in_specs=(
            P(None, "leaf"),
            P(),
            P(),
            P(),
            P(),
            P(),
            P(),
            P(),
            P("leaf", None),
            P(None, "leaf"),
            P(None, "leaf"),
        ),
        out_specs=P(None, "leaf"),
        check_vma=False,
    )
```

```python
import functools

import jax
import jax.numpy as jnp
from jax import lax
from jax.experimental import pallas as pl
from jax.experimental.pallas import tpu as pltpu
from jax.sharding import PartitionSpec as P

HALO = 32
PEERS = 4
CAP_FAR = 32
LANES = 128
BF = jnp.bfloat16
F32 = jnp.float32
MESH = pl.DeviceIdType.MESH
OFFSETS = tuple(range(-PEERS, 0)) + tuple(range(1, PEERS + 1))


def mm(a, b):
    return jnp.dot(a, b, preferred_element_type=F32)


def halves(x):
    high = x.astype(BF)
    return high, (x - high.astype(F32)).astype(BF)


def one_hot(rows, index):
    count = index.shape[1]
    lines = lax.broadcasted_iota(jnp.int32, (rows, count), 0).astype(F32).astype(BF)
    hit = lines == jnp.broadcast_to(index.astype(BF), (rows, count))
    return jnp.where(hit, jnp.ones((), BF), jnp.zeros((), BF))


def kernel(
    n, cells, cap,
    slip_ref, tm_ref, up_ref, down_ref, sib_ref, leaf_ref, ts_ref, nb_ref, send_ref, far_ref, near_ref,
    out_ref,
    outgoing, far_buf, near_buf, edges, halo, root_out, roots,
    weight, w_up, w_sib, w_down, agg, terms, loc, rel, near_rel, source, leaf_cat, columns,
    far_send, far_recv, near_send, near_recv, halo_send, halo_recv, root_send, root_recv,
):
    me = lax.axis_index("leaf")
    coef = tm_ref.shape[0]
    types = far_ref.shape[0]
    kinds = near_ref.shape[0]
    rest = cap - CAP_FAR

    barrier = pltpu.get_barrier_semaphore()

    far_buf[...] = jnp.zeros_like(far_buf)
    near_buf[...] = jnp.zeros_like(near_buf)
    halo[...] = jnp.zeros_like(halo)

    def greet(k, carry):
        pl.semaphore_signal(barrier, inc=1, device_id=(lax.rem(me + k, n),), device_id_type=MESH)
        return carry

    lax.fori_loop(1, n, greet, 0)

    edges[0] = slip_ref[:, :LANES].astype(F32).T[:HALO].astype(BF)
    edges[1] = slip_ref[:, cells - LANES :].astype(F32).T[LANES - HALO :].astype(BF)

    weight[...] = jnp.zeros_like(weight)
    weight[0, :coef, :] = tm_ref[...].astype(F32)
    multipole = mm(weight[0].astype(BF), slip_ref[...]).astype(BF)
    source[:, :cells] = multipole

    def far_copy(k):
        target = lax.rem(me + k, n)
        return pltpu.make_async_remote_copy(
            src_ref=outgoing.at[pl.ds(pl.multiple_of(target * cap, cap), CAP_FAR)],
            dst_ref=far_buf.at[pl.ds(pl.multiple_of(me * CAP_FAR, CAP_FAR), CAP_FAR)],
            send_sem=far_send.at[k],
            recv_sem=far_recv.at[k],
            device_id=(target,),
            device_id_type=MESH,
        )

    def near_copy(j):
        target = jnp.clip(me + OFFSETS[j], 0, n - 1)
        back = len(OFFSETS) - 1 - j
        return pltpu.make_async_remote_copy(
            src_ref=outgoing.at[pl.ds(pl.multiple_of(target * cap + CAP_FAR, CAP_FAR), rest)],
            dst_ref=near_buf.at[pl.ds(back * rest, rest)],
            send_sem=near_send.at[j],
            recv_sem=near_recv.at[back],
            device_id=(target,),
            device_id_type=MESH,
        )

    def halo_copy(side):
        target = jnp.clip(me + (1 if side else -1), 0, n - 1)
        return pltpu.make_async_remote_copy(
            src_ref=edges.at[side],
            dst_ref=halo.at[pl.ds((1 - side) * HALO, HALO)],
            send_sem=halo_send.at[side],
            recv_sem=halo_recv.at[1 - side],
            device_id=(target,),
            device_id_type=MESH,
        )

    def root_copy(k):
        return pltpu.make_async_remote_copy(
            src_ref=root_out,
            dst_ref=roots.at[pl.ds(pl.multiple_of(me * 8, 8), 8)],
            send_sem=root_send.at[k],
            recv_sem=root_recv.at[k],
            device_id=(lax.rem(me + k, n),),
            device_id_type=MESH,
        )

    def inside(offset):
        return jnp.logical_and(me + offset >= 0, me + offset < n)

    def parts(ref, index):
        weight[index, :coef, :coef] = ref
        weight[index, :coef, coef:] = jnp.zeros((coef, LANES - coef), F32)
        return halves(weight[index].T)

    w_sib[...] = jnp.zeros_like(w_sib)
    for s in (0, 1):
        high, low = parts(up_ref[:, s, :], 0 + s)
        w_up[s * LANES : (s + 1) * LANES, :LANES] = high
        w_up[s * LANES : (s + 1) * LANES, LANES:] = low
        high, low = parts(down_ref[:, s, :], 2 + s)
        w_down[:LANES, s * LANES : (s + 1) * LANES] = high
        w_down[LANES:, s * LANES : (s + 1) * LANES] = low
        high, low = parts(sib_ref[:, s, :], 4 + s)
        other = 1 - s
        w_sib[0, other * LANES : (other + 1) * LANES, s * LANES : (s + 1) * LANES] = high
        w_sib[1, other * LANES : (other + 1) * LANES, s * LANES : (s + 1) * LANES] = low

    def pair(base, rows):
        m = max(rows // 2, 8)
        even = agg[pl.ds(base, m, stride=2), :]
        odd = agg[pl.ds(base + 1, m, stride=2), :]
        return m, halves(jnp.concatenate([even, odd], axis=1))

    def lift(high, low):
        first = mm(high, w_up[...])
        second = mm(low, w_up[:, :LANES])
        return first[:, :LANES] + first[:, LANES:] + second

    def across(high, low):
        return mm(high, w_sib[0]) + mm(high, w_sib[1]) + mm(low, w_sib[0])

    def place(base, value):
        agg[base : base + value.shape[0], :] = value
        if value.shape[0] < 16:
            agg[base + value.shape[0] : base + 16, :] = jnp.zeros((16 - value.shape[0], LANES), F32)

    local_levels = cells.bit_length() - 1
    tree_bits = n.bit_length() - 1
    base, spot = 0, 0
    agg[:cells, :] = multipole.astype(F32).T
    local_spots = []
    for height in range(local_levels):
        rows = cells >> height
        m, (high, low) = pair(base, rows)
        if height >= 1:
            terms[spot : spot + m, :] = across(high, low)
            local_spots.append(spot)
            spot += m
        else:
            local_spots.append(None)
        value = lift(high, low)
        base += max(rows, 16)
        place(base, value)
    root_out[...] = value
    roots[pl.ds(pl.multiple_of(me * 8, 8), 8), :] = value

    chunk = 4 * cap
    for start in range(0, n * cap, chunk):
        picked = one_hot(cells, send_ref[0:1, start : start + chunk].astype(F32))
        outgoing[start : start + chunk, :] = mm(multipole, picked).T.astype(BF)

    pl.semaphore_wait(barrier, n - 1)

    def start_root(k, carry):
        root_copy(k).start()
        return carry

    lax.fori_loop(1, n, start_root, 0)
    for side in (0, 1):
        @pl.when(inside(1 if side else -1))
        def _():
            halo_copy(side).start()

    def start_far(k, carry):
        far_copy(k).start()
        return carry

    lax.fori_loop(1, n, start_far, 0)
    for j, offset in enumerate(OFFSETS):
        @pl.when(inside(offset))
        def _():
            near_copy(j).start()

    v = far_ref[...]
    behind = v - cells
    sender = behind // cap
    slot = behind % cap
    delta = sender - me
    lane = jnp.where(delta < 0, delta + PEERS, delta + PEERS - 1)
    position = jnp.where(
        v < cells,
        v,
        jnp.where(
            slot < CAP_FAR,
            cells + near_buf.shape[0] + sender * CAP_FAR + slot,
            cells + lane * rest + slot - CAP_FAR,
        ),
    )
    total = source.shape[1]
    blocks = total // 256
    for b in range(blocks):
        rel[b, :types, :] = jnp.clip(position - 256 * b, -1, 256).astype(F32)

    for side in (0, 1):
        @pl.when(inside(1 if side else -1))
        def _():
            halo_copy(side).wait_send()

        @pl.when(inside(-1 if side else 1))
        def _():
            halo_copy(side).wait_recv()

    w = near_ref[...]
    near_rel[0, :kinds, :] = jnp.clip(w - HALO, -1, cells).astype(F32)
    near_rel[1, :kinds, :] = jnp.where(
        w < HALO, w, jnp.where(w >= HALO + cells, w - cells, -1)
    ).astype(F32)
    slips = slip_ref[...]
    side_slips = jnp.concatenate(
        [halo[...], jnp.zeros((LANES - 2 * HALO, LANES), BF)], axis=0
    ).astype(F32).T.astype(BF)
    stress = jnp.zeros(out_ref.shape, F32)
    for k in range(kinds):
        column = mm(slips, one_hot(cells, near_rel[0, k : k + 1, :])) + mm(
            side_slips, one_hot(LANES, near_rel[1, k : k + 1, :])
        )
        stress = stress + mm(nb_ref[k], column.astype(BF))
    out_ref[...] = stress

    leaf_cat[...] = jnp.zeros_like(leaf_cat)
    for t in range(types):
        leaf_cat[:coef, t * LANES : t * LANES + coef] = leaf_ref[t]

    for j, offset in enumerate(OFFSETS):
        @pl.when(inside(offset))
        def _():
            near_copy(j).wait_send()

        @pl.when(inside(OFFSETS[len(OFFSETS) - 1 - j]))
        def _():
            near_copy(j).wait_recv()

    close = cells + near_buf.shape[0]
    source[:, cells:close] = near_buf[...].astype(F32).T.astype(BF)
    group = 3 if types % 3 == 0 else 1

    def gather(low, high, more):
        def step(g, carry):
            for i in range(group):
                t = g * group + i
                hits = jnp.concatenate(
                    [one_hot(256, rel[b, pl.ds(t, 1), :]) for b in range(low, high)], axis=0
                )
                picked = mm(source[:, low * 256 : high * 256], hits).astype(BF)
                rows = pl.ds(pl.multiple_of(t * LANES, LANES), LANES)
                if more:
                    picked = picked + columns[rows, :]
                columns[rows, :] = picked
            return carry

        lax.fori_loop(0, types // group, step, 0)

    gather(0, close // 256, False)

    def wait_root(k, carry):
        root_copy(k).wait()
        return carry

    lax.fori_loop(1, n, wait_root, 0)
    base = 0
    place(base, roots[pl.ds(0, n, stride=8), :])
    tree_spots = []
    for bit in range(tree_bits):
        rows = n >> bit
        m, (high, low) = pair(base, rows)
        terms[spot : spot + m, :] = across(high, low)
        tree_spots.append(spot)
        spot += m
        if bit + 1 < tree_bits:
            value = lift(high, low)
            base += max(rows, 16)
            place(base, value)

    def descend(x):
        high, low = halves(x)
        return mm(high, w_down[:LANES, :]) + mm(high, w_down[LANES:, :]) + mm(low, w_down[:LANES, :])

    expansion = jnp.zeros((8, LANES), F32)
    for bit in reversed(range(tree_bits)):
        both = terms[pl.ds(tree_spots[bit] + (me >> (bit + 1)), 1), :]
        both = jnp.broadcast_to(both, (8, 2 * LANES))
        if bit + 1 < tree_bits:
            both = both + descend(expansion)
        expansion = jnp.where((me >> bit) & 1 == 0, both[:, :LANES], both[:, LANES:])
    for height in reversed(range(local_levels)):
        m = max((cells >> height) // 2, 8)
        both = descend(expansion)
        if height >= 1:
            both = both + terms[local_spots[height] : local_spots[height] + m, :]
        loc[pl.ds(0, m, stride=2), :] = both[:, :LANES]
        loc[pl.ds(1, m, stride=2), :] = both[:, LANES:]
        expansion = loc[: max(cells >> height, 8), :]

    def wait_far(k, carry):
        far_copy(k).wait()
        return carry

    lax.fori_loop(1, n, wait_far, 0)
    source[:, close:] = far_buf[...].astype(F32).T.astype(BF)
    gather(close // 256, blocks, True)
    leaf_sum = mm(leaf_cat[...], columns[...])
    local_exp = (expansion.T + leaf_sum)[:coef].astype(BF)
    out_ref[...] = out_ref[...] + mm(ts_ref[...], local_exp)


def round_up(value, unit):
    return -(-value // unit) * unit


def body(*args):
    slip, to_multipole, _, _, _, _, _, _, send_cells, far_list, near_list = args
    n = lax.axis_size("leaf")
    cells = slip.shape[1]
    cap = send_cells.shape[1] // n
    rest = cap - CAP_FAR
    peers = len(OFFSETS)
    total = cells + n * CAP_FAR + peers * rest
    dma = pltpu.SemaphoreType.DMA
    return pl.pallas_call(
        functools.partial(kernel, n, cells, cap),
        out_shape=jax.ShapeDtypeStruct(slip.shape, F32),
        in_specs=[pl.BlockSpec(memory_space=pltpu.VMEM)] * len(args),
        out_specs=pl.BlockSpec(memory_space=pltpu.VMEM),
        scratch_shapes=[
            pltpu.VMEM((n * cap, LANES), BF),
            pltpu.VMEM((n * CAP_FAR, LANES), BF),
            pltpu.VMEM((peers * rest, LANES), BF),
            pltpu.VMEM((2, HALO, LANES), BF),
            pltpu.VMEM((2 * HALO, LANES), BF),
            pltpu.VMEM((8, LANES), F32),
            pltpu.VMEM((n * 8, LANES), F32),
            pltpu.VMEM((6, LANES, LANES), F32),
            pltpu.VMEM((2 * LANES, 2 * LANES), BF),
            pltpu.VMEM((2, 2 * LANES, 2 * LANES), BF),
            pltpu.VMEM((2 * LANES, 2 * LANES), BF),
            pltpu.VMEM((2 * cells + 2 * n + 128, LANES), F32),
            pltpu.VMEM((cells + n + 128, 2 * LANES), F32),
            pltpu.VMEM((cells, LANES), F32),
            pltpu.VMEM((total // 256, round_up(far_list.shape[0], 8), cells), F32),
            pltpu.VMEM((2, round_up(near_list.shape[0], 8), cells), F32),
            pltpu.VMEM((LANES, total), BF),
            pltpu.VMEM((LANES, far_list.shape[0] * LANES), BF),
            pltpu.VMEM((far_list.shape[0] * LANES, cells), BF),
            dma((n,)),
            dma((n,)),
            dma((peers,)),
            dma((peers,)),
            dma((2,)),
            dma((2,)),
            dma((n,)),
            dma((n,)),
        ],
        compiler_params=pltpu.CompilerParams(collective_id=0, has_side_effects=True),
    )(*(jnp.transpose(a, (1, 0, 2)) if 2 <= i < 5 else a for i, a in enumerate(args)))


def solution(mesh):
    return jax.shard_map(
        body,
        mesh=mesh,
        in_specs=(
            P(None, "leaf"),
            P(),
            P(),
            P(),
            P(),
            P(),
            P(),
            P(),
            P("leaf", None),
            P(None, "leaf"),
            P(None, "leaf"),
        ),
        out_specs=P(None, "leaf"),
        check_vma=False,
    )
```

```python
import functools

import jax
import jax.numpy as jnp
from jax import lax
from jax.experimental import pallas as pl
from jax.experimental.pallas import tpu as pltpu
from jax.sharding import PartitionSpec as P

HALO = 32
PEERS = 4
CAP_FAR = 32
LANES = 128
BF = jnp.bfloat16
F32 = jnp.float32
MESH = pl.DeviceIdType.MESH
OFFSETS = tuple(range(-PEERS, 0)) + tuple(range(1, PEERS + 1))


def mm(a, b):
    return jnp.dot(a, b, preferred_element_type=F32)


def halves(x):
    high = x.astype(BF)
    return high, (x - high.astype(F32)).astype(BF)


def one_hot(rows, index):
    count = index.shape[1]
    lines = lax.broadcasted_iota(jnp.int32, (rows, count), 0).astype(F32).astype(BF)
    hit = lines == jnp.broadcast_to(index.astype(BF), (rows, count))
    return jnp.where(hit, jnp.ones((), BF), jnp.zeros((), BF))


def kernel(
    n, cells, cap,
    slip_ref, tm_ref, up_ref, down_ref, sib_ref, leaf_any, ts_ref, nb_any, send_ref, far_ref, near_ref,
    out_ref,
    outgoing, far_buf, near_buf, edges, halo, root_out, roots,
    weight, w_up, w_sib, w_down, agg, terms, loc, rel, near_rel, source, leaf_cat, columns, near_cols, leaf_ref, nb_ref, load_sem,
    far_send, far_recv, near_send, near_recv, halo_send, halo_recv, root_send, root_recv,
):
    me = lax.axis_index("leaf")
    coef = tm_ref.shape[0]
    types = far_ref.shape[0]
    kinds = near_ref.shape[0]
    rest = cap - CAP_FAR

    loads = (
        pltpu.make_async_copy(leaf_any, leaf_ref, load_sem.at[0]),
        pltpu.make_async_copy(nb_any, nb_ref, load_sem.at[1]),
    )
    for copy in loads:
        copy.start()

    barrier = pltpu.get_barrier_semaphore()

    far_buf[...] = jnp.zeros_like(far_buf)
    near_buf[...] = jnp.zeros_like(near_buf)
    halo[...] = jnp.zeros_like(halo)

    def greet(k, carry):
        pl.semaphore_signal(barrier, inc=1, device_id=(lax.rem(me + k, n),), device_id_type=MESH)
        return carry

    lax.fori_loop(1, n, greet, 0)

    edges[0] = slip_ref[:, :LANES].astype(F32).T[:HALO].astype(BF)
    edges[1] = slip_ref[:, cells - LANES :].astype(F32).T[LANES - HALO :].astype(BF)

    weight[...] = jnp.zeros_like(weight)
    weight[0, :coef, :] = tm_ref[...].astype(F32)
    multipole = mm(weight[0].astype(BF), slip_ref[...]).astype(BF)
    source[:, :cells] = multipole

    def far_copy(k):
        target = lax.rem(me + k, n)
        return pltpu.make_async_remote_copy(
            src_ref=outgoing.at[pl.ds(pl.multiple_of(target * cap, cap), CAP_FAR)],
            dst_ref=far_buf.at[pl.ds(pl.multiple_of(me * CAP_FAR, CAP_FAR), CAP_FAR)],
            send_sem=far_send.at[k],
            recv_sem=far_recv.at[k],
            device_id=(target,),
            device_id_type=MESH,
        )

    def near_copy(j):
        target = jnp.clip(me + OFFSETS[j], 0, n - 1)
        back = len(OFFSETS) - 1 - j
        return pltpu.make_async_remote_copy(
            src_ref=outgoing.at[pl.ds(pl.multiple_of(target * cap + CAP_FAR, CAP_FAR), rest)],
            dst_ref=near_buf.at[pl.ds(back * rest, rest)],
            send_sem=near_send.at[j],
            recv_sem=near_recv.at[back],
            device_id=(target,),
            device_id_type=MESH,
        )

    def halo_copy(side):
        target = jnp.clip(me + (1 if side else -1), 0, n - 1)
        return pltpu.make_async_remote_copy(
            src_ref=edges.at[side],
            dst_ref=halo.at[pl.ds((1 - side) * HALO, HALO)],
            send_sem=halo_send.at[side],
            recv_sem=halo_recv.at[1 - side],
            device_id=(target,),
            device_id_type=MESH,
        )

    def root_copy(k):
        return pltpu.make_async_remote_copy(
            src_ref=root_out,
            dst_ref=roots.at[me],
            send_sem=root_send.at[k],
            recv_sem=root_recv.at[k],
            device_id=(lax.rem(me + k, n),),
            device_id_type=MESH,
        )

    def inside(offset):
        return jnp.logical_and(me + offset >= 0, me + offset < n)

    def parts(ref, index):
        weight[index, :coef, :coef] = ref
        weight[index, :coef, coef:] = jnp.zeros((coef, LANES - coef), F32)
        return halves(weight[index].T)

    w_sib[...] = jnp.zeros_like(w_sib)
    for s in (0, 1):
        high, low = parts(up_ref[:, s, :], 0 + s)
        w_up[s * LANES : (s + 1) * LANES, :LANES] = high
        w_up[s * LANES : (s + 1) * LANES, LANES:] = low
        high, low = parts(down_ref[:, s, :], 2 + s)
        w_down[:LANES, s * LANES : (s + 1) * LANES] = high
        w_down[LANES:, s * LANES : (s + 1) * LANES] = low
        high, low = parts(sib_ref[:, s, :], 4 + s)
        other = 1 - s
        w_sib[0, other * LANES : (other + 1) * LANES, s * LANES : (s + 1) * LANES] = high
        w_sib[1, other * LANES : (other + 1) * LANES, s * LANES : (s + 1) * LANES] = low

    def pair(base, rows):
        m = max(rows // 2, 8)
        even = agg[pl.ds(base, m, stride=2), :]
        odd = agg[pl.ds(base + 1, m, stride=2), :]
        return m, halves(jnp.concatenate([even, odd], axis=1))

    def lift(high, low):
        first = mm(high, w_up[...])
        second = mm(low, w_up[:, :LANES])
        return first[:, :LANES] + first[:, LANES:] + second

    def across(high, low):
        return mm(high, w_sib[0]) + mm(high, w_sib[1]) + mm(low, w_sib[0])

    def place(base, value):
        agg[base : base + value.shape[0], :] = value
        if value.shape[0] < 16:
            agg[base + value.shape[0] : base + 16, :] = jnp.zeros((16 - value.shape[0], LANES), F32)

    local_levels = cells.bit_length() - 1
    tree_bits = n.bit_length() - 1
    base, spot = 0, 0
    agg[:cells, :] = multipole.astype(F32).T
    local_spots = []
    for height in range(local_levels):
        rows = cells >> height
        m, (high, low) = pair(base, rows)
        if height >= 1:
            terms[spot : spot + m, :] = across(high, low)
            local_spots.append(spot)
            spot += m
        else:
            local_spots.append(None)
        value = lift(high, low)
        base += max(rows, 16)
        place(base, value)
    root_out[...] = value[:1]
    roots[me] = value[:1]

    chunk = 4 * cap
    for start in range(0, n * cap, chunk):
        picked = one_hot(cells, send_ref[0:1, start : start + chunk].astype(F32))
        outgoing[start : start + chunk, :] = mm(multipole, picked).T.astype(BF)

    v = far_ref[...]
    behind = v - cells
    sender = behind // cap
    slot = behind % cap
    delta = sender - me
    lane = jnp.where(delta < 0, delta + PEERS, delta + PEERS - 1)
    position = jnp.where(
        v < cells,
        v,
        jnp.where(
            slot < CAP_FAR,
            cells + near_buf.shape[0] + sender * CAP_FAR + slot,
            cells + lane * rest + slot - CAP_FAR,
        ),
    )
    total = source.shape[1]
    blocks = total // 256
    for b in range(blocks):
        rel[b, :types, :] = jnp.clip(position - 256 * b, -1, 256).astype(F32)

    w = near_ref[...]
    near_rel[0, :kinds, :] = jnp.clip(w - HALO, -1, cells).astype(F32)
    near_rel[1, :kinds, :] = jnp.where(
        w < HALO, w, jnp.where(w >= HALO + cells, w - cells, -1)
    ).astype(F32)
    slips = slip_ref[...]
    for k in range(kinds):
        near_cols[k * LANES : (k + 1) * LANES, :] = mm(
            slips, one_hot(cells, near_rel[0, k : k + 1, :])
        ).astype(BF)

    group = 3 if types % 3 == 0 else 1

    def gather(low, high, more):
        def step(g, carry):
            for i in range(group):
                t = g * group + i
                hits = jnp.concatenate(
                    [one_hot(256, rel[b, pl.ds(t, 1), :]) for b in range(low, high)], axis=0
                )
                picked = mm(source[:, low * 256 : high * 256], hits).astype(BF)
                rows = pl.ds(pl.multiple_of(t * LANES, LANES), LANES)
                if more:
                    picked = picked + columns[rows, :]
                columns[rows, :] = picked
            return carry

        lax.fori_loop(0, types // group, step, 0)

    gather(0, cells // 256, False)

    for copy in loads:
        copy.wait()
    leaf_cat[...] = jnp.zeros_like(leaf_cat)
    for t in range(types):
        leaf_cat[:coef, t * LANES : t * LANES + coef] = leaf_ref[t]

    pl.semaphore_wait(barrier, n - 1)

    def start_root(k, carry):
        root_copy(k).start()
        return carry

    lax.fori_loop(1, n, start_root, 0)
    for side in (0, 1):
        @pl.when(inside(1 if side else -1))
        def _():
            halo_copy(side).start()

    for j, offset in enumerate(OFFSETS):
        @pl.when(inside(offset))
        def _():
            near_copy(j).start()
    def start_far(k, carry):
        far_copy(lax.rem(k + n // 2 - 2, n - 1) + 1).start()
        return carry

    lax.fori_loop(1, n, start_far, 0)

    for j, offset in enumerate(OFFSETS):
        @pl.when(inside(offset))
        def _():
            near_copy(j).wait_send()

        @pl.when(inside(OFFSETS[len(OFFSETS) - 1 - j]))
        def _():
            near_copy(j).wait_recv()

    close = cells + near_buf.shape[0]
    source[:, cells:close] = near_buf[...].astype(F32).T.astype(BF)
    gather(cells // 256, close // 256, True)

    for side in (0, 1):
        @pl.when(inside(1 if side else -1))
        def _():
            halo_copy(side).wait_send()

        @pl.when(inside(-1 if side else 1))
        def _():
            halo_copy(side).wait_recv()

    side_slips = jnp.concatenate(
        [halo[...], jnp.zeros((LANES - 2 * HALO, LANES), BF)], axis=0
    ).astype(F32).T.astype(BF)
    stress = jnp.zeros(out_ref.shape, F32)
    for k in range(kinds):
        column = near_cols[k * LANES : (k + 1) * LANES, :] + mm(
            side_slips, one_hot(LANES, near_rel[1, k : k + 1, :])
        ).astype(BF)
        stress = stress + mm(nb_ref[k], column)
    out_ref[...] = stress

    def wait_root(k, carry):
        root_copy(k).wait()
        return carry

    lax.fori_loop(1, n, wait_root, 0)
    base = 0
    place(base, roots[:, 0, :])
    tree_spots = []
    for bit in range(tree_bits):
        rows = n >> bit
        m, (high, low) = pair(base, rows)
        terms[spot : spot + m, :] = across(high, low)
        tree_spots.append(spot)
        spot += m
        if bit + 1 < tree_bits:
            value = lift(high, low)
            base += max(rows, 16)
            place(base, value)

    def descend(x):
        high, low = halves(x)
        return mm(high, w_down[:LANES, :]) + mm(high, w_down[LANES:, :]) + mm(low, w_down[:LANES, :])

    expansion = jnp.zeros((8, LANES), F32)
    for bit in reversed(range(tree_bits)):
        both = terms[pl.ds(tree_spots[bit] + (me >> (bit + 1)), 1), :]
        both = jnp.broadcast_to(both, (8, 2 * LANES))
        if bit + 1 < tree_bits:
            both = both + descend(expansion)
        expansion = jnp.where((me >> bit) & 1 == 0, both[:, :LANES], both[:, LANES:])
    for height in reversed(range(local_levels)):
        m = max((cells >> height) // 2, 8)
        both = descend(expansion)
        if height >= 1:
            both = both + terms[local_spots[height] : local_spots[height] + m, :]
        loc[pl.ds(0, m, stride=2), :] = both[:, :LANES]
        loc[pl.ds(1, m, stride=2), :] = both[:, LANES:]
        expansion = loc[: max(cells >> height, 8), :]

    def wait_far(k, carry):
        far_copy(k).wait()
        return carry

    lax.fori_loop(1, n, wait_far, 0)
    source[:, close:] = far_buf[...].astype(F32).T.astype(BF)
    gather(close // 256, blocks, True)
    leaf_sum = mm(leaf_cat[...], columns[...])
    local_exp = (expansion.T + leaf_sum)[:coef].astype(BF)
    out_ref[...] = out_ref[...] + mm(ts_ref[...], local_exp)


def round_up(value, unit):
    return -(-value // unit) * unit


def body(*args):
    slip, _, _, _, _, leaf_far, _, near_blocks, send_cells, far_list, near_list = args
    n = lax.axis_size("leaf")
    cells = slip.shape[1]
    cap = send_cells.shape[1] // n
    rest = cap - CAP_FAR
    peers = len(OFFSETS)
    total = cells + n * CAP_FAR + peers * rest
    dma = pltpu.SemaphoreType.DMA
    return pl.pallas_call(
        functools.partial(kernel, n, cells, cap),
        out_shape=jax.ShapeDtypeStruct(slip.shape, F32),
        in_specs=[
            pl.BlockSpec(memory_space=pl.ANY if i in (5, 7) else pltpu.VMEM) for i in range(len(args))
        ],
        out_specs=pl.BlockSpec(memory_space=pltpu.VMEM),
        scratch_shapes=[
            pltpu.VMEM((n * cap, LANES), BF),
            pltpu.VMEM((n * CAP_FAR, LANES), BF),
            pltpu.VMEM((peers * rest, LANES), BF),
            pltpu.VMEM((2, HALO, LANES), BF),
            pltpu.VMEM((2 * HALO, LANES), BF),
            pltpu.VMEM((1, LANES), F32),
            pltpu.VMEM((n, 1, LANES), F32),
            pltpu.VMEM((6, LANES, LANES), F32),
            pltpu.VMEM((2 * LANES, 2 * LANES), BF),
            pltpu.VMEM((2, 2 * LANES, 2 * LANES), BF),
            pltpu.VMEM((2 * LANES, 2 * LANES), BF),
            pltpu.VMEM((2 * cells + 2 * n + 128, LANES), F32),
            pltpu.VMEM((cells + n + 128, 2 * LANES), F32),
            pltpu.VMEM((cells, LANES), F32),
            pltpu.VMEM((total // 256, round_up(far_list.shape[0], 8), cells), F32),
            pltpu.VMEM((2, round_up(near_list.shape[0], 8), cells), F32),
            pltpu.VMEM((LANES, total), BF),
            pltpu.VMEM((LANES, far_list.shape[0] * LANES), BF),
            pltpu.VMEM((far_list.shape[0] * LANES, cells), BF),
            pltpu.VMEM((near_list.shape[0] * LANES, cells), BF),
            pltpu.VMEM(leaf_far.shape, BF),
            pltpu.VMEM(near_blocks.shape, BF),
            dma((2,)),
            dma((n,)),
            dma((n,)),
            dma((peers,)),
            dma((peers,)),
            dma((2,)),
            dma((2,)),
            dma((n,)),
            dma((n,)),
        ],
        compiler_params=pltpu.CompilerParams(collective_id=0, has_side_effects=True),
    )(*(jnp.transpose(a, (1, 0, 2)) if 2 <= i < 5 else a for i, a in enumerate(args)))


def solution(mesh):
    return jax.shard_map(
        body,
        mesh=mesh,
        in_specs=(
            P(None, "leaf"),
            P(),
            P(),
            P(),
            P(),
            P(),
            P(),
            P(),
            P("leaf", None),
            P(None, "leaf"),
            P(None, "leaf"),
        ),
        out_specs=P(None, "leaf"),
        check_vma=False,
    )
```
